32 devices in a mesh: row: 8 (over y, x, core), col: 4 (over z).
Axes of the slice: x: 2, y: 2, z: 4, core: 2. Of those that a mesh axis runs over, the one named last changes fastest.
Arguments:
- blocks: bfloat16 [8, 4, 368, 128, 128], P('row', 'col'), may hold values from -0.125 to 0.125
- block_rows: int32 [8, 4, 368], P('row', 'col'), may hold values from 0 to 31, as said below
- block_cols: int32 [8, 4, 368], P('row', 'col'), may hold values from 0 to 63
- counts: int32 [8, 4], P('row', 'col'), may hold values from 1 to 368, as said below
- features: bfloat16 [32768, 256], P(('col', 'row')), may hold values from -6 to 6
Outputs:
- aggregated: bfloat16 [32768, 256], P(('row', 'col'))
The draws below stay inside these ranges and needn't reach their ends.
Inputs may be any that keep to these rules, and one draw needn't show every extreme that they name: `block_rows`: within one tile the live slots name distinct pairs of block row and block column. `counts`: some tile holds exactly 368 live blocks in every draw.
All inputs are finite; a program needn't handle non-finite values.
Results may differ from the reference program's by a relative error of at most 0.013.
Values may be sent and summed in bfloat16 or wider, within the bound.
A program may use at most 128 MiB of HBM per device.

```python
import jax
import jax.numpy as jnp
from jax import lax

F = 256
BS = 128
Q = 8
MAXB = 368
BR = 32
BC = 64
NB = 256
NODES = 32768
N_ROW = 8
N_COL = 4


def pattern_draw(key):
    base_key = jax.random.fold_in(key, 7)
    slot_key = jax.random.fold_in(base_key, 1)
    count_key = jax.random.fold_in(base_key, 2)
    chosen_key = jax.random.fold_in(base_key, 3)
    tile_total = N_ROW * N_COL
    tile_keys = jax.random.split(slot_key, tile_total)
    slot_ids = jax.vmap(lambda tile_key: jax.random.permutation(tile_key, BR * BC)[:MAXB])(tile_keys)
    slot_ids = slot_ids.astype(jnp.int32).reshape(N_ROW, N_COL, MAXB)
    raw_draw = jax.random.randint(count_key, (tile_total,), 0, MAXB + 1, dtype=jnp.int32)
    tile_counts = jnp.maximum(raw_draw * raw_draw // MAXB, 1)
    chosen_tile = jax.random.randint(chosen_key, (), 0, tile_total, dtype=jnp.int32)
    tile_counts = jnp.where(jnp.arange(tile_total, dtype=jnp.int32) == chosen_tile, MAXB, tile_counts)
    return (slot_ids // BC, slot_ids % BC, tile_counts.reshape(N_ROW, N_COL).astype(jnp.int32))


def draw_block_rows(key, part):
    return pattern_draw(key)[0]


def draw_block_cols(key, part):
    return pattern_draw(key)[1]


def draw_counts(key, part):
    return pattern_draw(key)[2]


def level_of(stream_key, extent, pieces, smallest, top_value):
    def one(position, shards_of):
        draws = jax.random.uniform(jax.random.fold_in(jax.random.fold_in(stream_key, 6), position), (shards_of,), jnp.float32, smallest / len(pieces), top_value / len(pieces))
        return jnp.repeat(jnp.exp(draws), extent[position] // shards_of).reshape((-1,) + (1,) * (len(extent) - position - 1))

    factor_of = one(*pieces[0])
    for cut in pieces[1:]:
        factor_of = factor_of * one(*cut)
    return factor_of


def noise(key, shape, spread, limit, pieces=(), kind=jnp.bfloat16):
    result = jax.random.normal(key, shape, jnp.float32) * spread
    if len(pieces) > 0:
        result = level_of(key, shape, pieces, -0.22, 0.18) * result
    return jnp.clip(result, min=-limit, max=limit).astype(kind)


def setup_inputs(seed: int = 0) -> dict:
    seeds = jax.random.split(jax.random.key(seed), 6)
    return {
        "blocks": noise(seeds[0], (N_ROW, N_COL, MAXB, BS, BS), (BS * MAXB // (3 * Q)) ** -0.5, 0.125, ((0, 8), (1, 4))),
        "block_rows": draw_block_rows(jax.random.fold_in(seeds[5], 71), 0),
        "block_cols": draw_block_cols(jax.random.fold_in(seeds[5], 71), 0),
        "counts": draw_counts(jax.random.fold_in(seeds[5], 71), 0),
        "features": noise(seeds[4], (NODES, F), 1.0, 6.0, ((0, 32),)),
    }


def reference(blocks, block_rows, block_cols, counts, features):
    feature_blocks = features.reshape(NB, BS, F)

    def per_tile(running, tile_index):
        row_panel = tile_index // N_COL
        col_panel = tile_index % N_COL
        tile_blocks = blocks[row_panel, col_panel]
        tile_rows = block_rows[row_panel, col_panel]
        tile_cols = block_cols[row_panel, col_panel]
        live_mask = jnp.arange(MAXB, dtype=jnp.int32) < counts[row_panel, col_panel]
        gathered = feature_blocks[(col_panel * BC + tile_cols).astype(jnp.int32)]
        product = jnp.einsum("gik,gkf->gif", tile_blocks.astype(jnp.float32), gathered.astype(jnp.float32))
        product = jnp.where(live_mask[:, None, None], product, jnp.float32(0.0))
        partial_value = jnp.zeros((BR, BS, F), jnp.float32).at[tile_rows.astype(jnp.int32)].add(product)
        rounded = lax.optimization_barrier(partial_value.astype(jnp.bfloat16)).astype(jnp.float32)
        start = (row_panel * BR).astype(jnp.int32)
        zero = jnp.int32(0)
        current = lax.dynamic_slice(running, (start, zero, zero), (BR, BS, F))
        running = lax.dynamic_update_slice(running, current + rounded, (start, zero, zero))
        return running, None

    initial = jnp.zeros((NB, BS, F), jnp.float32)
    running, _ = lax.scan(per_tile, initial, jnp.arange(N_ROW * N_COL, dtype=jnp.int32))
    return running.reshape(NB * BS, F).astype(jnp.bfloat16)
```

```python
import functools

import jax
import jax.numpy as jnp
from jax import lax
from jax.experimental import pallas as pl
from jax.experimental.pallas import tpu as pltpu
from jax.sharding import PartitionSpec as P

MESH = pl.DeviceIdType.MESH
LANES = 128
HALVES = 2


def bits_for(extent):
    return max(1, (extent - 1).bit_length())


def slot_plan(tile_rows, tile_cols, live_count, row_blocks, slot_bits, col_bits):
    slots = tile_rows.shape[0]
    position = jnp.arange(slots, dtype=jnp.int32)
    row = jnp.where(position < live_count, tile_rows, row_blocks)
    key = (row << slot_bits) + position
    rank = jnp.sum((key[None, :] < key[:, None]).astype(jnp.int32), axis=1)
    packed = (key << col_bits) + tile_cols
    ordered = jnp.sum(jnp.where(rank[:, None] == position[None, :], packed[:, None], 0), axis=0)
    wanted = jnp.arange(row_blocks, dtype=jnp.int32)
    upto = jnp.sum((row[:, None] <= wanted[None, :]).astype(jnp.int32), axis=0)
    here = jnp.sum((row[:, None] == wanted[None, :]).astype(jnp.int32), axis=0)
    last = jnp.where(here > 0, upto - 1, -1)
    return ordered, last


def kernel(
    n_row, n_col, row_blocks, slot_bits, col_bits,
    ordered, last, blocks_hbm, features_hbm, out,
    held, panel0, panel1, sums, part0, part1, right0, right1, left0, left1,
    load_sem, ag_send, ag_recv, rs_send, rs_recv,
):
    panels, parts = (panel0, panel1), (part0, part1)
    rights, lefts = (right0, right1), (left0, left1)
    slots = held.shape[0]
    owned = panel0.shape[0] // n_row
    chunk = row_blocks // n_col
    me = lax.axis_index("row")
    p = lax.axis_index("col")

    fetch = pltpu.make_async_copy(blocks_hbm, held, load_sem.at[HALVES])
    mine = [
        pltpu.make_async_copy(
            features_hbm.at[:, :, pl.ds(h * LANES, LANES)],
            panels[h].at[pl.ds(me * owned, owned)],
            load_sem.at[h],
        )
        for h in range(HALVES)
    ]
    for copy in mine:
        copy.start()
    fetch.start()

    cube = n_row == 8
    core = lax.rem(me, 2)
    if cube:
        x_bit = lax.rem(me // 2, 2)
        y_bit = me // 4
        other = me + 1 - 2 * core
        beside = me + 2 - 4 * x_bit
        above = me + 4 - 8 * y_bit
        across = beside + 4 - 8 * y_bit
        flip = 1 - 2 * core
        mates = [other, beside, above]
    else:
        mates = [lax.rem(me + k, n_row) for k in range(1, n_row)]

    barrier = pltpu.get_barrier_semaphore()
    for mate in mates:
        pl.semaphore_signal(barrier, inc=1, device_id=(mate, p), device_id_type=MESH)

    @pl.when(p > 0)
    def _():
        pl.semaphore_signal(barrier, inc=1, device_id=(me, p - 1), device_id_type=MESH)

    @pl.when(p < n_col - 1)
    def _():
        pl.semaphore_signal(barrier, inc=1, device_id=(me, p + 1), device_id_type=MESH)

    inner = jnp.logical_and(p > 0, p < n_col - 1)

    @pl.when(inner)
    def _():
        pl.semaphore_wait(barrier, len(mates) + 2)

    @pl.when(jnp.logical_not(inner))
    def _():
        pl.semaphore_wait(barrier, len(mates) + 1)

    def shard_copy(h, shard, target, send, recv):
        where = panels[h].at[pl.ds(shard * owned, owned)]
        return pltpu.make_async_remote_copy(
            src_ref=where,
            dst_ref=where,
            send_sem=ag_send.at[h, send],
            recv_sem=ag_recv.at[h, recv],
            device_id=(target, p),
            device_id_type=MESH,
        )

    if cube:
        def first_sends(h):
            shard_copy(h, me, beside, 0, 0).start()
            shard_copy(h, me, above, 1, 1).start()
            shard_copy(h, me, other, 2, 3).start()

        def forward(h):
            @pl.when(core == 0)
            def _():
                shard_copy(h, above, me, 1, 1).wait_recv()
                shard_copy(h, above, beside, 3, 2).start()
                shard_copy(h, above, other, 5, 5).start()
                shard_copy(h, beside, me, 0, 0).wait_recv()
                shard_copy(h, beside, other, 4, 4).start()

            @pl.when(core == 1)
            def _():
                shard_copy(h, beside, me, 0, 0).wait_recv()
                shard_copy(h, beside, above, 3, 2).start()
                shard_copy(h, beside, other, 4, 4).start()
                shard_copy(h, above, me, 1, 1).wait_recv()
                shard_copy(h, above, other, 5, 5).start()

        def gathered(h):
            shard_copy(h, across, me, 2, 2).wait_recv()
            shard_copy(h, across, other, 6, 6).start()
            shard_copy(h, other, me, 2, 3).wait_recv()
            shard_copy(h, beside + flip, me, 4, 4).wait_recv()
            shard_copy(h, above + flip, me, 5, 5).wait_recv()
            shard_copy(h, across + flip, me, 6, 6).wait_recv()

        sends = 7
    else:
        def first_sends(h):
            for k in range(1, n_row):
                shard_copy(h, me, lax.rem(me + k, n_row), k - 1, k - 1).start()

        def forward(h):
            pass

        def gathered(h):
            for k in range(1, n_row):
                shard_copy(h, lax.rem(me + n_row - k, n_row), me, k - 1, k - 1).wait_recv()

        sends = n_row - 1

    def compute(h):
        unroll = 8 if slots % 8 == 0 else 1

        def step(group, carry):
            total, before = carry
            for u in range(unroll):
                place = group * unroll + u
                word = ordered[place]
                row = word >> (slot_bits + col_bits)
                slot = (word >> col_bits) & ((1 << slot_bits) - 1)
                col = word & ((1 << col_bits) - 1)
                product = jnp.dot(held[slot], panels[h][col], preferred_element_type=jnp.float32)
                total = jnp.where(row == before, total, 0.0) + product
                sums[place] = total.astype(jnp.bfloat16)
                before = row
            return total, before

        zero = jnp.zeros((held.shape[1], LANES), jnp.float32)
        lax.fori_loop(0, slots // unroll, step, (zero, jnp.int32(-1)))

        def pick(i, _):
            place = last[i]
            value = sums[jnp.maximum(place, 0)]
            parts[h][i] = jnp.where(place >= 0, value, jnp.zeros_like(value))
            return 0

        lax.fori_loop(0, row_blocks, pick, 0)

    def rs_copy(h, side, d, source):
        land = (rights, lefts)[side][h]
        return pltpu.make_async_remote_copy(
            src_ref=source,
            dst_ref=land.at[d],
            send_sem=rs_send.at[h, side, d],
            recv_sem=rs_recv.at[h, side, d],
            device_id=(me, p + 1 - 2 * side),
            device_id_type=MESH,
        )

    def own(h, d):
        return parts[h].at[pl.ds(d * chunk, chunk)]

    def start_ends(h):
        @pl.when(p == 0)
        def _():
            for d in range(n_col - 1, 0, -1):
                rs_copy(h, 0, d, own(h, d)).start()

        @pl.when(p == n_col - 1)
        def _():
            for d in range(n_col - 1):
                rs_copy(h, 1, d, own(h, d)).start()

    def pass_on(h, side, d):
        land = (rights, lefts)[side][h]
        rs_copy(h, side, d, land.at[d]).wait_recv()

        def add(k, _):
            land[d, k] = (
                land[d, k].astype(jnp.float32) + parts[h][d * chunk + k].astype(jnp.float32)
            ).astype(jnp.bfloat16)
            return 0

        lax.fori_loop(0, chunk, add, 0)
        rs_copy(h, side, d, land.at[d]).start()

    def relay(h):
        for k in range(n_col - 1):
            d = n_col - 1 - k

            @pl.when(jnp.logical_and(p > 0, p < d))
            def _():
                pass_on(h, 0, d)

            @pl.when(jnp.logical_and(p > k, p < n_col - 1))
            def _():
                pass_on(h, 1, k)

    def finish(h):
        cols = pl.ds(h * LANES, LANES)

        def total(from_left, from_right):
            if from_left:
                rs_copy(h, 0, p, rights[h].at[p]).wait_recv()
            if from_right:
                rs_copy(h, 1, p, lefts[h].at[p]).wait_recv()

            def add(k, _):
                value = parts[h][p * chunk + k].astype(jnp.float32)
                if from_left:
                    value = value + rights[h][p, k].astype(jnp.float32)
                if from_right:
                    value = value + lefts[h][p, k].astype(jnp.float32)
                out[k, :, cols] = value.astype(jnp.bfloat16)
                return 0

            lax.fori_loop(0, chunk, add, 0)

        pl.when(p == 0)(lambda: total(False, True))
        pl.when(p == n_col - 1)(lambda: total(True, False))
        pl.when(jnp.logical_and(p > 0, p < n_col - 1))(lambda: total(True, True))

    for h in range(HALVES):
        mine[h].wait()
        first_sends(h)
    forward(0)
    gathered(0)
    fetch.wait()
    compute(0)
    start_ends(0)
    forward(1)
    gathered(1)
    compute(1)
    start_ends(1)
    for h in range(HALVES):
        relay(h)
        finish(h)

    for h in range(HALVES):
        for k in range(sends):
            shard_copy(h, me, me, k, 0).wait_send()
        for d in range(n_col):
            @pl.when(p < d)
            def _():
                rs_copy(h, 0, d, own(h, d)).wait_send()

            @pl.when(p > d)
            def _():
                rs_copy(h, 1, d, own(h, d)).wait_send()


def on_device(n_row, n_col, blocks, block_rows, block_cols, counts, features):
    nodes, width = features.shape
    slots, size = blocks.shape[2], blocks.shape[-1]
    owned = nodes // size
    row_blocks = n_col * owned
    panel_blocks = n_row * owned
    slot_bits, col_bits = bits_for(slots), bits_for(panel_blocks)
    ordered, last = slot_plan(
        block_rows[0, 0], block_cols[0, 0], counts[0, 0], row_blocks, slot_bits, col_bits
    )
    half = (size, LANES)
    vmem = lambda *lead: pltpu.VMEM((*lead, *half), jnp.bfloat16)
    smem = pl.BlockSpec(memory_space=pltpu.SMEM)
    hbm = pl.BlockSpec(memory_space=pl.ANY)
    result = pl.pallas_call(
        functools.partial(kernel, n_row, n_col, row_blocks, slot_bits, col_bits),
        out_shape=jax.ShapeDtypeStruct((owned, size, width), jnp.bfloat16),
        in_specs=[smem, smem, hbm, hbm],
        out_specs=pl.BlockSpec(memory_space=pltpu.VMEM),
        scratch_shapes=[
            pltpu.VMEM((slots, size, size), jnp.bfloat16),
            vmem(panel_blocks), vmem(panel_blocks),
            vmem(slots),
            vmem(row_blocks), vmem(row_blocks),
            vmem(n_col, owned), vmem(n_col, owned), vmem(n_col, owned), vmem(n_col, owned),
            pltpu.SemaphoreType.DMA((HALVES + 1,)),
            pltpu.SemaphoreType.DMA((HALVES, max(7, n_row - 1))),
            pltpu.SemaphoreType.DMA((HALVES, max(7, n_row - 1))),
            pltpu.SemaphoreType.DMA((HALVES, 2, n_col)),
            pltpu.SemaphoreType.DMA((HALVES, 2, n_col)),
        ],
        compiler_params=pltpu.CompilerParams(
            collective_id=0, has_side_effects=True, vmem_limit_bytes=67043328
        ),
    )(ordered, last, blocks.reshape(slots, size, size), features.reshape(owned, size, width))
    return result.reshape(nodes, width)


def solution(mesh):
    return jax.shard_map(
        functools.partial(on_device, mesh.shape["row"], mesh.shape["col"]),
        mesh=mesh,
        in_specs=(
            P("row", "col", None, None, None),
            P("row", "col", None),
            P("row", "col", None),
            P("row", "col"),
            P(("col", "row"), None),
        ),
        out_specs=P(("row", "col"), None),
        check_vma=False,
    )
```

```python
import functools

import jax
import jax.numpy as jnp
from jax import lax
from jax.experimental import pallas as pl
from jax.experimental.pallas import tpu as pltpu
from jax.sharding import PartitionSpec as P

MESH = pl.DeviceIdType.MESH
LANES = 128
HALVES = 2


def bits_for(extent):
    return max(1, (extent - 1).bit_length())


def slot_plan(tile_rows, tile_cols, live_count, row_blocks, slot_bits, col_bits):
    slots = tile_rows.shape[0]
    position = jnp.arange(slots, dtype=jnp.int32)
    row = jnp.where(position < live_count, tile_rows, row_blocks)
    key = (row << slot_bits) + position
    rank = jnp.sum((key[None, :] < key[:, None]).astype(jnp.int32), axis=1)
    packed = (key << col_bits) + tile_cols
    ordered = jnp.sum(jnp.where(rank[:, None] == position[None, :], packed[:, None], 0), axis=0)
    wanted = jnp.arange(row_blocks, dtype=jnp.int32)
    upto = jnp.sum((row[:, None] <= wanted[None, :]).astype(jnp.int32), axis=0)
    here = jnp.sum((row[:, None] == wanted[None, :]).astype(jnp.int32), axis=0)
    last = jnp.where(here > 0, upto - 1, -1)
    return ordered, last


def kernel(
    n_row, n_col, row_blocks, slot_bits, col_bits,
    ordered, last, blocks_hbm, features_hbm, out,
    held, panel0, panel1, sums, part0, part1, right0, right1, left0, left1,
    load_sem, ag_send, ag_recv, rs_send, rs_recv,
):
    panels, parts = (panel0, panel1), (part0, part1)
    rights, lefts = (right0, right1), (left0, left1)
    slots = held.shape[0]
    owned = panel0.shape[0] // n_row
    chunk = row_blocks // n_col
    me = lax.axis_index("row")
    p = lax.axis_index("col")

    fetch = pltpu.make_async_copy(blocks_hbm, held, load_sem.at[HALVES])
    mine = [
        pltpu.make_async_copy(
            features_hbm.at[:, :, pl.ds(h * LANES, LANES)],
            panels[h].at[pl.ds(me * owned, owned)],
            load_sem.at[h],
        )
        for h in range(HALVES)
    ]
    for copy in mine:
        copy.start()
    fetch.start()

    cube = n_row == 8
    core = lax.rem(me, 2)
    if cube:
        x_bit = lax.rem(me // 2, 2)
        y_bit = me // 4
        other = me + 1 - 2 * core
        beside = me + 2 - 4 * x_bit
        above = me + 4 - 8 * y_bit
        across = beside + 4 - 8 * y_bit
        flip = 1 - 2 * core
        mates = [other, beside, above]
    else:
        mates = [lax.rem(me + k, n_row) for k in range(1, n_row)]

    barrier = pltpu.get_barrier_semaphore()
    for mate in mates:
        pl.semaphore_signal(barrier, inc=1, device_id=(mate, p), device_id_type=MESH)

    @pl.when(p > 0)
    def _():
        pl.semaphore_signal(barrier, inc=1, device_id=(me, p - 1), device_id_type=MESH)

    @pl.when(p < n_col - 1)
    def _():
        pl.semaphore_signal(barrier, inc=1, device_id=(me, p + 1), device_id_type=MESH)

    inner = jnp.logical_and(p > 0, p < n_col - 1)

    @pl.when(inner)
    def _():
        pl.semaphore_wait(barrier, len(mates) + 2)

    @pl.when(jnp.logical_not(inner))
    def _():
        pl.semaphore_wait(barrier, len(mates) + 1)

    def shard_copy(h, shard, target, send, recv):
        where = panels[h].at[pl.ds(shard * owned, owned)]
        return pltpu.make_async_remote_copy(
            src_ref=where,
            dst_ref=where,
            send_sem=ag_send.at[h, send],
            recv_sem=ag_recv.at[h, recv],
            device_id=(target, p),
            device_id_type=MESH,
        )

    if cube:
        def first_sends(h):
            shard_copy(h, me, beside, 0, 0).start()
            shard_copy(h, me, above, 1, 1).start()
            shard_copy(h, me, other, 2, 3).start()

        def forward(h):
            @pl.when(core == 0)
            def _():
                shard_copy(h, above, me, 1, 1).wait_recv()
                shard_copy(h, above, beside, 3, 2).start()
                shard_copy(h, above, other, 5, 5).start()
                shard_copy(h, beside, me, 0, 0).wait_recv()
                shard_copy(h, beside, other, 4, 4).start()

            @pl.when(core == 1)
            def _():
                shard_copy(h, beside, me, 0, 0).wait_recv()
                shard_copy(h, beside, above, 3, 2).start()
                shard_copy(h, beside, other, 4, 4).start()
                shard_copy(h, above, me, 1, 1).wait_recv()
                shard_copy(h, above, other, 5, 5).start()

        def gathered(h):
            shard_copy(h, across, me, 2, 2).wait_recv()
            shard_copy(h, across, other, 6, 6).start()
            shard_copy(h, other, me, 2, 3).wait_recv()
            shard_copy(h, beside + flip, me, 4, 4).wait_recv()
            shard_copy(h, above + flip, me, 5, 5).wait_recv()
            shard_copy(h, across + flip, me, 6, 6).wait_recv()

        sends = 7
    else:
        def first_sends(h):
            for k in range(1, n_row):
                shard_copy(h, me, lax.rem(me + k, n_row), k - 1, k - 1).start()

        def forward(h):
            pass

        def gathered(h):
            for k in range(1, n_row):
                shard_copy(h, lax.rem(me + n_row - k, n_row), me, k - 1, k - 1).wait_recv()

        sends = n_row - 1

    def compute(h):
        unroll = 8 if slots % 8 == 0 else 1

        def step(group, carry):
            total, before = carry
            for u in range(unroll):
                place = group * unroll + u
                word = ordered[place]
                row = word >> (slot_bits + col_bits)
                slot = (word >> col_bits) & ((1 << slot_bits) - 1)
                col = word & ((1 << col_bits) - 1)
                product = jnp.dot(held[slot], panels[h][col], preferred_element_type=jnp.float32)
                total = jnp.where(row == before, total, 0.0) + product
                sums[place] = total.astype(jnp.bfloat16)
                before = row
            return total, before

        zero = jnp.zeros((held.shape[1], LANES), jnp.float32)
        lax.fori_loop(0, slots // unroll, step, (zero, jnp.int32(-1)))

        def pick(i, _):
            place = last[i]
            value = sums[jnp.maximum(place, 0)]
            parts[h][i] = jnp.where(place >= 0, value, jnp.zeros_like(value))
            return 0

        lax.fori_loop(0, row_blocks, pick, 0)

    def rs_copy(h, side, d, source):
        land = (rights, lefts)[side][h]
        return pltpu.make_async_remote_copy(
            src_ref=source,
            dst_ref=land.at[d],
            send_sem=rs_send.at[h, side, d],
            recv_sem=rs_recv.at[h, side, d],
            device_id=(me, p + 1 - 2 * side),
            device_id_type=MESH,
        )

    def own(h, d):
        return parts[h].at[pl.ds(d * chunk, chunk)]

    def start_ends(h):
        @pl.when(p == 0)
        def _():
            for d in range(n_col - 1, 0, -1):
                rs_copy(h, 0, d, own(h, d)).start()

        @pl.when(p == n_col - 1)
        def _():
            for d in range(n_col - 1):
                rs_copy(h, 1, d, own(h, d)).start()

    def pass_on(h, side, d):
        land = (rights, lefts)[side][h]
        rs_copy(h, side, d, land.at[d]).wait_recv()

        def add(k, _):
            land[d, k] = (
                land[d, k].astype(jnp.float32) + parts[h][d * chunk + k].astype(jnp.float32)
            ).astype(jnp.bfloat16)
            return 0

        lax.fori_loop(0, chunk, add, 0)
        rs_copy(h, side, d, land.at[d]).start()

    def relay(h):
        for k in range(n_col - 1):
            d = n_col - 1 - k

            relays_left = jnp.logical_and(p > k, p < n_col - 1)
            near_end = p >= n_col // 2

            @pl.when(jnp.logical_and(relays_left, near_end))
            def _():
                pass_on(h, 1, k)

            @pl.when(jnp.logical_and(p > 0, p < d))
            def _():
                pass_on(h, 0, d)

            @pl.when(jnp.logical_and(relays_left, jnp.logical_not(near_end)))
            def _():
                pass_on(h, 1, k)

    def finish(h):
        cols = pl.ds(h * LANES, LANES)

        def total(from_left, from_right):
            if from_left:
                rs_copy(h, 0, p, rights[h].at[p]).wait_recv()
            if from_right:
                rs_copy(h, 1, p, lefts[h].at[p]).wait_recv()

            def add(k, _):
                value = parts[h][p * chunk + k].astype(jnp.float32)
                if from_left:
                    value = value + rights[h][p, k].astype(jnp.float32)
                if from_right:
                    value = value + lefts[h][p, k].astype(jnp.float32)
                out[k, :, cols] = value.astype(jnp.bfloat16)
                return 0

            lax.fori_loop(0, chunk, add, 0)

        pl.when(p == 0)(lambda: total(False, True))
        pl.when(p == n_col - 1)(lambda: total(True, False))
        pl.when(jnp.logical_and(p > 0, p < n_col - 1))(lambda: total(True, True))

    mine[0].wait()
    first_sends(0)
    forward(0)
    mine[1].wait()
    first_sends(1)
    gathered(0)
    fetch.wait()
    compute(0)
    start_ends(0)
    forward(1)
    gathered(1)
    compute(1)
    start_ends(1)
    for h in range(HALVES):
        relay(h)
    for h in range(HALVES):
        finish(h)

    for h in range(HALVES):
        for k in range(sends):
            shard_copy(h, me, me, k, 0).wait_send()
        for d in range(n_col):
            @pl.when(p < d)
            def _():
                rs_copy(h, 0, d, own(h, d)).wait_send()

            @pl.when(p > d)
            def _():
                rs_copy(h, 1, d, own(h, d)).wait_send()


def on_device(n_row, n_col, blocks, block_rows, block_cols, counts, features):
    nodes, width = features.shape
    slots, size = blocks.shape[2], blocks.shape[-1]
    owned = nodes // size
    row_blocks = n_col * owned
    panel_blocks = n_row * owned
    slot_bits, col_bits = bits_for(slots), bits_for(panel_blocks)
    ordered, last = slot_plan(
        block_rows[0, 0], block_cols[0, 0], counts[0, 0], row_blocks, slot_bits, col_bits
    )
    half = (size, LANES)
    vmem = lambda *lead: pltpu.VMEM((*lead, *half), jnp.bfloat16)
    smem = pl.BlockSpec(memory_space=pltpu.SMEM)
    hbm = pl.BlockSpec(memory_space=pl.ANY)
    result = pl.pallas_call(
        functools.partial(kernel, n_row, n_col, row_blocks, slot_bits, col_bits),
        out_shape=jax.ShapeDtypeStruct((owned, size, width), jnp.bfloat16),
        in_specs=[smem, smem, hbm, hbm],
        out_specs=pl.BlockSpec(memory_space=pltpu.VMEM),
        scratch_shapes=[
            pltpu.VMEM((slots, size, size), jnp.bfloat16),
            vmem(panel_blocks), vmem(panel_blocks),
            vmem(slots),
            vmem(row_blocks), vmem(row_blocks),
            vmem(n_col, owned), vmem(n_col, owned), vmem(n_col, owned), vmem(n_col, owned),
            pltpu.SemaphoreType.DMA((HALVES + 1,)),
            pltpu.SemaphoreType.DMA((HALVES, max(7, n_row - 1))),
            pltpu.SemaphoreType.DMA((HALVES, max(7, n_row - 1))),
            pltpu.SemaphoreType.DMA((HALVES, 2, n_col)),
            pltpu.SemaphoreType.DMA((HALVES, 2, n_col)),
        ],
        compiler_params=pltpu.CompilerParams(
            collective_id=0, has_side_effects=True, vmem_limit_bytes=67043328
        ),
    )(ordered, last, blocks.reshape(slots, size, size), features.reshape(owned, size, width))
    return result.reshape(nodes, width)


def solution(mesh):
    return jax.shard_map(
        functools.partial(on_device, mesh.shape["row"], mesh.shape["col"]),
        mesh=mesh,
        in_specs=(
            P("row", "col", None, None, None),
            P("row", "col", None),
            P("row", "col", None),
            P("row", "col"),
            P(("col", "row"), None),
        ),
        out_specs=P(("row", "col"), None),
        check_vma=False,
    )
```
